32 devices in a mesh: rows: 16 (over z, y, x), cols: 2 (over core).
Axes of the slice: x: 2, y: 2, z: 4, core: 2. Of those that a mesh axis runs over, the one named last changes fastest.
Arguments:
- embeddings: bfloat16 [49152, 1536], P('rows'), may hold values from -43 to 43, as said below
- start_basis: float32 [1536, 256], P(None, 'cols'), may hold values from -6 to 6
Outputs:
- projected: bfloat16 [49152, 256], P('rows', 'cols')
- basis: float32 [1536, 256], P(None, 'cols')
The draws below stay inside these ranges and needn't reach their ends.
Inputs may be any that keep to these rules, and one draw needn't show every extreme that they name: `embeddings`: rows are noisy vectors around offsets that differ between aligned blocks of rows, with per-column spreads that differ by a factor of up to four.
All inputs are finite; a program needn't handle non-finite values.
Results may differ from the reference program's by a relative error of at most 0.025.
Values may be sent and summed in bfloat16 or wider, within the bound.
No kernel may reach another device: no remote copies, remote signals or barrier semaphores. Data moves between devices by JAX's collectives and lax.ppermute only.
A program may use at most 64 MiB of HBM per device.

```python
import jax
import jax.numpy as jnp
from jax import lax

D = 1536
K = 256
ROW_DEV = 3072
ITERS = 3
ROWS = 49152


def draw_embeddings(key, part):
    key_offset, key_scale, key_noise = jax.random.split(key, 3)
    key_blocks = jax.random.fold_in(key, 7919)
    offset = jnp.clip(jax.random.normal(key_offset, (D,), jnp.float32), -3.0, 3.0)
    col_scale = jnp.exp(jax.random.uniform(key_scale, (D,), jnp.float32, -0.69, 0.69))
    block_shift = jnp.clip(0.8 * jax.random.normal(key_blocks, (ROWS // ROW_DEV, D), jnp.float32), -3.0, 3.0)
    row_shift = jnp.repeat(block_shift, ROW_DEV, axis=0, total_repeat_length=ROWS)
    noise = jnp.clip(jax.random.normal(key_noise, (ROWS, D), jnp.float32), -5.0, 5.0)
    values = noise * col_scale[None, :] + offset[None, :] + row_shift
    return values.astype(jnp.bfloat16)


def block_scale(rng, extent, pieces, smallest, high):
    def one(dim, blocks):
        steps = jax.random.uniform(jax.random.fold_in(jax.random.fold_in(rng, 6), dim), (blocks,), jnp.float32, smallest / len(pieces), high / len(pieces))
        return jnp.repeat(jnp.exp(steps), extent[dim] // blocks).reshape((-1,) + (1,) * (len(extent) - dim - 1))

    gain = one(*pieces[0])
    for cut in pieces[1:]:
        gain = gain * one(*cut)
    return gain


def normal_values(own_key, shape, width, limit, cuts=(), held_as=jnp.bfloat16):
    values = width * jax.random.normal(own_key, shape, jnp.float32)
    if cuts:
        values = values * block_scale(own_key, shape, cuts, -0.22, 0.18)
    return jnp.clip(values, -limit, limit).astype(held_as)


def setup_inputs(seed: int = 0) -> dict:
    streams_of = jax.random.split(jax.random.key(seed), 3)
    return {
        "embeddings": draw_embeddings(jax.random.fold_in(streams_of[2], 71), 0),
        "start_basis": normal_values(streams_of[1], (D, K), 1.0, 6.0, ((1, 2),), jnp.float32),
    }


def reference(embeddings, start_basis):
    rows_count = embeddings.shape[0]
    col_mean = lax.optimization_barrier(jnp.sum(embeddings, axis=0, dtype=jnp.float32)) / rows_count
    basis = start_basis
    for sweep_index in range(ITERS):
        basis_bf = basis.astype(jnp.bfloat16)
        raw_proj = jnp.dot(embeddings.astype(jnp.float32), basis_bf.astype(jnp.float32), preferred_element_type=jnp.float32)
        offset = jnp.dot(col_mean, basis_bf.astype(jnp.float32), precision=lax.Precision.HIGHEST)
        shifted = (raw_proj - offset[None, :]).astype(jnp.bfloat16)
        col_sums = lax.optimization_barrier(jnp.sum(shifted, axis=0, dtype=jnp.float32))
        products = lax.dot_general(embeddings.astype(jnp.float32), shifted.astype(jnp.float32), (((0,), (0,)), ((), ())), preferred_element_type=jnp.float32)
        products = products - col_mean[:, None] * col_sums[None, :]
        gram_matrix = jnp.dot(products.T, products, precision=lax.Precision.HIGHEST)
        lower = jnp.linalg.cholesky(gram_matrix)
        basis = lax.linalg.triangular_solve(lower, products, left_side=False, lower=True, transpose_a=True)
    centered = embeddings.astype(jnp.float32) - col_mean[None, :]
    unit = (centered * lax.rsqrt(lax.optimization_barrier(jnp.sum(centered * centered, axis=1, keepdims=True)) + 1.0)).astype(jnp.bfloat16)
    coords = jnp.dot(unit.astype(jnp.float32), basis.astype(jnp.bfloat16).astype(jnp.float32), preferred_element_type=jnp.float32)
    scaled = coords * lax.rsqrt(lax.optimization_barrier(jnp.mean(coords * coords, axis=1, keepdims=True)) + 0.0001)
    return (scaled.astype(jnp.bfloat16), basis)
```

```python
import jax
import jax.numpy as jnp
from jax import lax
from jax.experimental import pallas as pl
from jax.experimental.pallas import tpu as pltpu
from jax.sharding import PartitionSpec as P

ITERS = 3
PANEL = 16
LANES = 128


def split3(x):
    hi = x.astype(jnp.bfloat16)
    rest = x - hi.astype(jnp.float32)
    mid = rest.astype(jnp.bfloat16)
    low = (rest - mid.astype(jnp.float32)).astype(jnp.bfloat16)
    return hi, mid, low


def inverse_factor_kernel(gram_ref, inv_ref, work_ref):
    size = gram_ref.shape[0]
    work_ref[...] = gram_ref[...]
    row = lax.broadcasted_iota(jnp.int32, (size, size), 0)
    col = lax.broadcasted_iota(jnp.int32, (size, size), 1)
    inv_ref[...] = (row == col).astype(jnp.float32)
    sub = lax.broadcasted_iota(jnp.int32, (PANEL, LANES), 0)
    chunks = size // LANES
    for start in range(0, size, PANEL):
        end = start + PANEL
        block = work_ref[start:end, :]
        first = start // LANES
        pieces = [work_ref[start:end, c * LANES : (c + 1) * LANES] for c in range(first, chunks)]
        count = len(pieces)
        pieces += [inv_ref[start:end, c * LANES : (c + 1) * LANES] for c in range(first + 1)]
        spread = [jnp.broadcast_to(block[:, start + k : start + k + 1], (PANEL, LANES)) for k in range(PANEL)]
        scale = jnp.ones((PANEL, LANES), jnp.float32)
        for k in range(PANEL):
            pivot = spread[k][k : k + 1, :]
            scale = jnp.where(sub == k, lax.rsqrt(pivot), scale)
            if k + 1 < PANEL:
                factor = jnp.where(sub > k, spread[k] * (1.0 / pivot), 0.0)
                pieces = [x - factor * x[k : k + 1, :] for x in pieces]
                spread = [x if i <= k else x - factor * x[k : k + 1, :] for i, x in enumerate(spread)]
        pieces = [x * scale for x in pieces]
        for i, c in enumerate(range(first + 1)):
            inv_ref[start:end, c * LANES : (c + 1) * LANES] = pieces[count + i]
        if end < size:
            hi, mid, low = split3(jnp.concatenate(pieces, axis=1))
            left = jnp.concatenate([hi, hi, mid, hi, low, mid], axis=0)[:, : count * LANES]
            right = jnp.concatenate([hi, mid, hi, low, hi, mid], axis=0)
            change = lax.dot_general(left, right, (((0,), (0,)), ((), ())), preferred_element_type=jnp.float32)
            change = change[end - first * LANES :, :]
            work_ref[end:, first * LANES :] = work_ref[end:, first * LANES :] - change[:, : count * LANES]
            done = (first + 1) * LANES
            inv_ref[end:, :done] = inv_ref[end:, :done] - change[:, count * LANES :]


def inverse_factor(gram):
    return pl.pallas_call(
        inverse_factor_kernel,
        out_shape=jax.ShapeDtypeStruct(gram.shape, jnp.float32),
        scratch_shapes=[pltpu.VMEM(gram.shape, jnp.float32)],
    )(gram)


def gather_rows(x):
    parts = lax.axis_size("rows")
    copies = jnp.broadcast_to(x[None], (parts,) + x.shape)
    return lax.all_to_all(copies, "rows", 0, 0)


def shards(embeddings, start_basis):
    f32, bf16 = jnp.float32, jnp.bfloat16
    local_rows, width = embeddings.shape
    row_parts = lax.axis_size("rows")
    col_parts = lax.axis_size("cols")
    row_index = lax.axis_index("rows")
    col_index = lax.axis_index("cols")
    col_block = start_basis.shape[1]
    basis_cols = col_block * col_parts
    half = width // col_parts
    piece = half // row_parts
    highest = lax.Precision.HIGHEST

    own_mean = jnp.sum(embeddings, axis=0, dtype=f32) / local_rows
    means = gather_rows(own_mean[None, :])[:, 0, :]
    col_mean = jnp.mean(means, axis=0)

    own_half = lax.dynamic_slice_in_dim(embeddings, col_index * half, half, 1)
    own_half_mean = lax.dynamic_slice_in_dim(own_mean, col_index * half, half, 0)
    second = lax.dot_general(own_half, embeddings, (((0,), (0,)), ((), ())), preferred_element_type=f32)
    within = (second - (local_rows * own_half_mean)[:, None] * own_mean[None, :]).astype(bf16)
    received = lax.all_to_all(within.reshape(row_parts, piece, width), "rows", 0, 0)
    between = means - col_mean[None, :]
    own_between = lax.dynamic_slice_in_dim(between, col_index * half + row_index * piece, piece, 1)
    scatter = jnp.sum(received.astype(f32), axis=0) + local_rows * lax.dot_general(
        own_between, between, (((0,), (0,)), ((), ())), precision=highest
    )

    basis = lax.all_gather(start_basis.astype(bf16), "cols", axis=1, tiled=True)
    next_piece = jnp.dot(scatter, basis.astype(f32), precision=highest)
    for sweep_index in range(ITERS):
        own_products = gather_rows(next_piece.astype(bf16)).reshape(half, basis_cols)
        products = lax.all_gather(own_products, "cols", axis=0, tiled=True)
        gram_matrix = lax.dot_general(products, products, (((0,), (0,)), ((), ())), preferred_element_type=f32)
        inverse = inverse_factor(gram_matrix)
        if sweep_index + 1 < ITERS:
            mixed = jnp.dot(scatter, products.astype(f32), precision=highest)
            next_piece = lax.dot_general(mixed, inverse, (((1,), (1,)), ((), ())), precision=highest)
    basis = lax.dot_general(products.astype(f32), inverse, (((1,), (1,)), ((), ())), precision=highest)

    centered = embeddings.astype(f32) - col_mean[None, :]
    unit = (centered * lax.rsqrt(jnp.sum(centered * centered, axis=1, keepdims=True) + 1.0)).astype(bf16)
    coords = jnp.dot(unit, basis.astype(bf16), preferred_element_type=f32)
    squares = jnp.sum(coords * coords, axis=1, keepdims=True)
    own_coords = lax.dynamic_slice_in_dim(coords, col_index * col_block, col_block, 1)
    scaled = own_coords * lax.rsqrt(squares / basis_cols + 0.0001)
    own_basis = lax.dynamic_slice_in_dim(basis, col_index * col_block, col_block, 1)
    return (scaled.astype(bf16), own_basis)


def solution(mesh):
    in_specs = (P("rows", None), P(None, "cols"))
    out_specs = (P("rows", "cols"), P(None, "cols"))
    return jax.shard_map(shards, mesh=mesh, in_specs=in_specs, out_specs=out_specs, check_vma=False)
```

```python
import jax
import jax.numpy as jnp
from jax import lax
from jax.experimental import pallas as pl
from jax.experimental.pallas import tpu as pltpu
from jax.sharding import PartitionSpec as P

ITERS = 3
PANEL = 16
LANES = 128


def split3(x):
    hi = x.astype(jnp.bfloat16)
    rest = x - hi.astype(jnp.float32)
    mid = rest.astype(jnp.bfloat16)
    low = (rest - mid.astype(jnp.float32)).astype(jnp.bfloat16)
    return hi, mid, low


def eliminate(inv_ref, work_ref):
    size = work_ref.shape[0]
    row = lax.broadcasted_iota(jnp.int32, (size, size), 0)
    col = lax.broadcasted_iota(jnp.int32, (size, size), 1)
    inv_ref[...] = (row == col).astype(jnp.float32)
    sub = lax.broadcasted_iota(jnp.int32, (PANEL, LANES), 0)
    chunks = size // LANES
    for start in range(0, size, PANEL):
        end = start + PANEL
        block = work_ref[start:end, :]
        first = start // LANES
        pieces = [work_ref[start:end, c * LANES : (c + 1) * LANES] for c in range(first, chunks)]
        count = len(pieces)
        pieces += [inv_ref[start:end, c * LANES : (c + 1) * LANES] for c in range(first + 1)]
        spread = [jnp.broadcast_to(block[:, start + k : start + k + 1], (PANEL, LANES)) for k in range(PANEL)]
        scale = jnp.ones((PANEL, LANES), jnp.float32)
        for k in range(PANEL):
            pivot = spread[k][k : k + 1, :]
            root = lax.rsqrt(pivot)
            scale = jnp.where(sub == k, root, scale)
            if k + 1 < PANEL:
                factor = jnp.where(sub > k, spread[k] * (root * root), 0.0)
                pieces = [x - factor * x[k : k + 1, :] for x in pieces]
                spread = [x if i <= k else x - factor * x[k : k + 1, :] for i, x in enumerate(spread)]
        pieces = [x * scale for x in pieces]
        for i, c in enumerate(range(first + 1)):
            inv_ref[start:end, c * LANES : (c + 1) * LANES] = pieces[count + i]
        if end < size:
            hi, mid, low = split3(jnp.concatenate(pieces, axis=1))
            left = jnp.concatenate([hi, hi, mid, hi, low, mid], axis=0)[:, : count * LANES]
            right = jnp.concatenate([hi, mid, hi, low, hi, mid], axis=0)
            change = lax.dot_general(left, right, (((0,), (0,)), ((), ())), preferred_element_type=jnp.float32)
            change = change[end - first * LANES :, :]
            work_ref[end:, first * LANES :] = work_ref[end:, first * LANES :] - change[:, : count * LANES]
            done = (first + 1) * LANES
            inv_ref[end:, :done] = inv_ref[end:, :done] - change[:, count * LANES :]


def gram_of(products):
    return lax.dot_general(products, products, (((0,), (0,)), ((), ())), preferred_element_type=jnp.float32)


def last_kernel(products_ref, inv_ref, work_ref):
    work_ref[...] = gram_of(products_ref[...])
    eliminate(inv_ref, work_ref)


def sweep_kernel(products_ref, scatter_ref, copies_ref, work_ref, inv_ref):
    products = products_ref[...]
    work_ref[...] = gram_of(products)
    rows = scatter_ref.shape[0]
    parts = jnp.dot(
        jnp.concatenate(split3(scatter_ref[...]), axis=0), products, preferred_element_type=jnp.float32
    )
    mixed = parts[:rows] + (parts[rows : 2 * rows] + parts[2 * rows :])
    eliminate(inv_ref, work_ref)
    following = lax.dot_general(
        mixed,
        inv_ref[...],
        (((1,), (1,)), ((), ())),
        precision=lax.Precision.HIGHEST,
        preferred_element_type=jnp.float32,
    ).astype(jnp.bfloat16)
    for i in range(copies_ref.shape[0]):
        copies_ref[i] = following[: copies_ref.shape[1]]


def inverse_factor(products):
    square = (products.shape[1], products.shape[1])
    return pl.pallas_call(
        last_kernel,
        out_shape=jax.ShapeDtypeStruct(square, jnp.float32),
        scratch_shapes=[pltpu.VMEM(square, jnp.float32)],
    )(products)


def next_copies(products, scatter, parts, piece):
    square = (products.shape[1], products.shape[1])
    return pl.pallas_call(
        sweep_kernel,
        out_shape=jax.ShapeDtypeStruct((parts, piece, products.shape[1]), jnp.bfloat16),
        scratch_shapes=[pltpu.VMEM(square, jnp.float32), pltpu.VMEM(square, jnp.float32)],
    )(products, scatter)


def gather_rows(x):
    parts = lax.axis_size("rows")
    return lax.all_to_all(jnp.broadcast_to(x[None], (parts,) + x.shape), "rows", 0, 0)


def shards(embeddings, start_basis):
    f32, bf16 = jnp.float32, jnp.bfloat16
    local_rows, width = embeddings.shape
    row_parts = lax.axis_size("rows")
    col_parts = lax.axis_size("cols")
    row_index = lax.axis_index("rows")
    col_index = lax.axis_index("cols")
    col_block = start_basis.shape[1]
    basis_cols = col_block * col_parts
    half = width // col_parts
    piece = half // row_parts
    highest = lax.Precision.HIGHEST

    own_mean = jnp.sum(embeddings, axis=0, dtype=f32) / local_rows
    means = gather_rows(own_mean[None, :])[:, 0, :]
    col_mean = jnp.mean(means, axis=0)

    own_half = lax.dynamic_slice_in_dim(embeddings, col_index * half, half, 1)
    own_half_mean = lax.dynamic_slice_in_dim(own_mean, col_index * half, half, 0)
    second = lax.dot_general(own_half, embeddings, (((0,), (0,)), ((), ())), preferred_element_type=f32)
    within = (second - (local_rows * own_half_mean)[:, None] * own_mean[None, :]).astype(bf16)
    received = lax.all_to_all(within.reshape(row_parts, piece, width), "rows", 0, 0)
    between = means - col_mean[None, :]
    own_between = lax.dynamic_slice_in_dim(between, col_index * half + row_index * piece, piece, 1)
    scatter = jnp.sum(received.astype(f32), axis=0) + local_rows * lax.dot_general(
        own_between, between, (((0,), (0,)), ((), ())), precision=highest
    )

    basis = lax.all_gather(start_basis.astype(bf16), "cols", axis=1, tiled=True)
    first = jnp.dot(scatter, basis.astype(f32), precision=highest).astype(bf16)
    copies = jnp.broadcast_to(first[None], (row_parts,) + first.shape)
    padded = jnp.pad(scatter, ((0, -piece % PANEL), (0, 0)))
    for sweep_index in range(ITERS):
        own_products = lax.all_to_all(copies, "rows", 0, 0).reshape(half, basis_cols)
        products = lax.all_gather(own_products, "cols", axis=0, tiled=True)
        if sweep_index + 1 < ITERS:
            copies = next_copies(products, padded, row_parts, piece)
    inverse = jnp.roll(inverse_factor(products), -col_index * col_block, axis=0)
    basis = lax.dot_general(products.astype(f32), inverse, (((1,), (1,)), ((), ())), precision=highest)

    centered = embeddings.astype(f32) - col_mean[None, :]
    unit = (centered * lax.rsqrt(jnp.sum(centered * centered, axis=1, keepdims=True) + 1.0)).astype(bf16)
    unit = lax.optimization_barrier(unit)
    coords = jnp.dot(unit, basis.astype(bf16), preferred_element_type=f32)
    squares = jnp.sum(coords * coords, axis=1, keepdims=True)
    scaled = coords[:, :col_block] * lax.rsqrt(squares / basis_cols + 0.0001)
    return (scaled.astype(bf16), basis[:, :col_block])


def solution(mesh):
    in_specs = (P("rows", None), P(None, "cols"))
    out_specs = (P("rows", "cols"), P(None, "cols"))
    return jax.shard_map(shards, mesh=mesh, in_specs=in_specs, out_specs=out_specs, check_vma=False)
```

```python
import jax
import jax.numpy as jnp
from jax import lax
from jax.experimental import pallas as pl
from jax.experimental.pallas import tpu as pltpu
from jax.sharding import PartitionSpec as P

ITERS = 3
PANEL = 16
CUTS = 2
LANES = 128


def split3(x):
    hi = x.astype(jnp.bfloat16)
    rest = x - hi.astype(jnp.float32)
    mid = rest.astype(jnp.bfloat16)
    low = (rest - mid.astype(jnp.float32)).astype(jnp.bfloat16)
    return hi, mid, low


def eliminate(inv_ref, work_ref):
    size = work_ref.shape[0]
    row = lax.broadcasted_iota(jnp.int32, (size, size), 0)
    col = lax.broadcasted_iota(jnp.int32, (size, size), 1)
    inv_ref[...] = (row == col).astype(jnp.float32)
    sub = lax.broadcasted_iota(jnp.int32, (PANEL, LANES), 0)
    chunks = size // LANES
    for start in range(0, size, PANEL):
        end = start + PANEL
        block = work_ref[start:end, :]
        first = start // LANES
        pieces = [work_ref[start:end, c * LANES : (c + 1) * LANES] for c in range(first, chunks)]
        count = len(pieces)
        pieces += [inv_ref[start:end, c * LANES : (c + 1) * LANES] for c in range(first + 1)]
        spread = [jnp.broadcast_to(block[:, start + k : start + k + 1], (PANEL, LANES)) for k in range(PANEL)]
        scale = jnp.ones((PANEL, LANES), jnp.float32)
        for k in range(PANEL):
            pivot = spread[k][k : k + 1, :]
            root = lax.rsqrt(pivot)
            scale = jnp.where(sub == k, root, scale)
            if k + 1 < PANEL:
                factor = jnp.where(sub > k, spread[k] * (root * root), 0.0)
                pieces = [x - factor * x[k : k + 1, :] for x in pieces]
                spread = [x if i <= k else x - factor * x[k : k + 1, :] for i, x in enumerate(spread)]
        pieces = [x * scale for x in pieces]
        for i, c in enumerate(range(first + 1)):
            inv_ref[start:end, c * LANES : (c + 1) * LANES] = pieces[count + i]
        if end < size:
            hi, mid, low = split3(jnp.concatenate(pieces, axis=1))
            left = jnp.concatenate([hi, hi, mid, hi, low, mid], axis=0)[:, : count * LANES]
            right = jnp.concatenate([hi, mid, hi, low, hi, mid], axis=0)
            change = lax.dot_general(left, right, (((0,), (0,)), ((), ())), preferred_element_type=jnp.float32)
            change = change[end - first * LANES :, :]
            work_ref[end:, first * LANES :] = work_ref[end:, first * LANES :] - change[:, : count * LANES]
            done = (first + 1) * LANES
            inv_ref[end:, :done] = inv_ref[end:, :done] - change[:, count * LANES :]


def gram_of(products):
    return lax.dot_general(products, products, (((0,), (0,)), ((), ())), preferred_element_type=jnp.float32)


def last_kernel(products_ref, inv_ref, work_ref):
    work_ref[...] = gram_of(products_ref[...])
    eliminate(inv_ref, work_ref)


def sweep_kernel(products_ref, scatter_ref, copies_ref, work_ref, inv_ref):
    products = products_ref[...]
    work_ref[...] = gram_of(products)
    rows = scatter_ref.shape[0]
    parts = jnp.dot(
        jnp.concatenate(split3(scatter_ref[...]), axis=0), products, preferred_element_type=jnp.float32
    )
    mixed = parts[:rows] + (parts[rows : 2 * rows] + parts[2 * rows :])
    eliminate(inv_ref, work_ref)
    following = lax.dot_general(
        mixed,
        inv_ref[...],
        (((1,), (1,)), ((), ())),
        precision=lax.Precision.HIGHEST,
        preferred_element_type=jnp.float32,
    ).astype(jnp.bfloat16)
    for i in range(copies_ref.shape[0]):
        copies_ref[i] = following[: copies_ref.shape[1]]


def inverse_factor(products):
    square = (products.shape[1], products.shape[1])
    return pl.pallas_call(
        last_kernel,
        out_shape=jax.ShapeDtypeStruct(square, jnp.float32),
        scratch_shapes=[pltpu.VMEM(square, jnp.float32)],
    )(products)


def next_copies(products, scatter, parts, piece):
    square = (products.shape[1], products.shape[1])
    return pl.pallas_call(
        sweep_kernel,
        out_shape=jax.ShapeDtypeStruct((parts, piece, products.shape[1]), jnp.bfloat16),
        scratch_shapes=[pltpu.VMEM(square, jnp.float32), pltpu.VMEM(square, jnp.float32)],
    )(products, scatter)


def gather_rows(x):
    parts = lax.axis_size("rows")
    return lax.all_to_all(jnp.broadcast_to(x[None], (parts,) + x.shape), "rows", 0, 0)


def shards(embeddings, start_basis):
    f32, bf16 = jnp.float32, jnp.bfloat16
    local_rows, width = embeddings.shape
    row_parts = lax.axis_size("rows")
    col_parts = lax.axis_size("cols")
    row_index = lax.axis_index("rows")
    col_index = lax.axis_index("cols")
    col_block = start_basis.shape[1]
    basis_cols = col_block * col_parts
    half = width // col_parts
    piece = half // row_parts
    highest = lax.Precision.HIGHEST

    own_mean = jnp.sum(embeddings, axis=0, dtype=f32) / local_rows
    means = gather_rows(own_mean[None, :])[:, 0, :]
    col_mean = jnp.mean(means, axis=0)

    own_half = lax.dynamic_slice_in_dim(embeddings, col_index * half, half, 1)
    own_half_mean = lax.dynamic_slice_in_dim(own_mean, col_index * half, half, 0)
    scaled_mean = (local_rows * own_half_mean)[:, None]
    received = []
    for cut in range(CUTS):
        span = slice(cut * width // CUTS, (cut + 1) * width // CUTS)
        second = lax.dot_general(
            own_half, embeddings[:, span], (((0,), (0,)), ((), ())), preferred_element_type=f32
        )
        within = (second - scaled_mean * own_mean[None, span]).astype(bf16)
        received.append(lax.all_to_all(within.reshape(row_parts, piece, -1), "rows", 0, 0))
    between = means - col_mean[None, :]
    own_between = lax.dynamic_slice_in_dim(between, col_index * half + row_index * piece, piece, 1)
    within_sum = jnp.concatenate([jnp.sum(x.astype(f32), axis=0) for x in received], axis=1)
    scatter = within_sum + local_rows * lax.dot_general(
        own_between, between, (((0,), (0,)), ((), ())), precision=highest
    )

    basis = lax.all_gather(start_basis.astype(bf16), "cols", axis=1, tiled=True)
    first = jnp.dot(scatter, basis.astype(f32), precision=highest).astype(bf16)
    copies = jnp.broadcast_to(first[None], (row_parts,) + first.shape)
    padded = jnp.pad(scatter, ((0, -piece % PANEL), (0, 0)))
    for sweep_index in range(ITERS):
        own_products = lax.all_to_all(copies, "rows", 0, 0).reshape(half, basis_cols)
        products = lax.all_gather(own_products, "cols", axis=0, tiled=True)
        if sweep_index + 1 < ITERS:
            copies = next_copies(products, padded, row_parts, piece)
    inverse = jnp.roll(inverse_factor(products), -col_index * col_block, axis=0)
    basis = lax.dot_general(products.astype(f32), inverse, (((1,), (1,)), ((), ())), precision=highest)

    centered = embeddings.astype(f32) - col_mean[None, :]
    unit = (centered * lax.rsqrt(jnp.sum(centered * centered, axis=1, keepdims=True) + 1.0)).astype(bf16)
    unit = lax.optimization_barrier(unit)
    coords = jnp.dot(unit, basis.astype(bf16), preferred_element_type=f32)
    squares = jnp.sum(coords * coords, axis=1, keepdims=True)
    scaled = coords[:, :col_block] * lax.rsqrt(squares / basis_cols + 0.0001)
    return (scaled.astype(bf16), basis[:, :col_block])


def solution(mesh):
    in_specs = (P("rows", None), P(None, "cols"))
    out_specs = (P("rows", "cols"), P(None, "cols"))
    return jax.shard_map(shards, mesh=mesh, in_specs=in_specs, out_specs=out_specs, check_vma=False)
```
